32 devices in a mesh: client: 16 (over z, y, core), tp: 2 (over x).
Axes of the slice: x: 2, y: 2, z: 4, core: 2. Of those that a mesh axis runs over, the one named last changes fastest.
Arguments:
- tokens: bfloat16 [4096, 2048], P('client'), may hold values from -6 to 6
- targets: bfloat16 [4096, 2048], P('client'), may hold values from -6 to 6
- norm_gain: float32 [2048], replicated, may hold values from 0.25 to 1.75
- up_frozen: bfloat16 [2048, 7168], P('client', 'tp'), may hold values from -0.125 to 0.125
- down_frozen: bfloat16 [7168, 2048], P('tp', 'client'), may hold values from -0.0625 to 0.0625
- up_left: float32 [16, 2048], replicated, may hold values from -1 to 1
- up_right: float32 [16, 7168], P(None, 'tp'), may hold values from -0.4375 to 0.4375
- down_left: float32 [16, 7168], P(None, 'tp'), may hold values from -0.625 to 0.625
- down_right: float32 [16, 2048], replicated, may hold values from -0.0625 to 0.0625
- counts: int32 [16], P('client'), may hold values from 64 to 4096
Outputs:
- round_up_left: float32 [16, 2048], replicated
- round_up_right: float32 [16, 7168], P(None, 'tp')
- round_down_left: float32 [16, 7168], P(None, 'tp')
- round_down_right: float32 [16, 2048], replicated
The draws below stay inside these ranges and needn't reach their ends.
All inputs are finite; a program needn't handle non-finite values.
Results may differ from the reference program's by a relative error of at most 0.0089.
Values may be sent and summed in bfloat16 or wider, within the bound.
A program may use at most 128 MiB of HBM per device.

```python
import jax
import jax.numpy as jnp
from jax import lax

D = 2048
FF = 7168
RANK = 16
TOK_CLIENT = 256
STEPS = 3
CLIENTS = 16
TOKENS = 4096
N_CLIENT = 16


def set_ends(result, own_key, smallest, high):
    place = [jax.random.randint(jax.random.fold_in(own_key, axis), (), 0, length) for axis, length in enumerate(result.shape)]
    widest = result.shape.index(max(result.shape))
    next_to = place[:widest] + [(place[widest] + 1) % result.shape[widest]] + place[widest + 1:]
    return result.at[tuple(place)].set(smallest).at[tuple(next_to)].set(high)


def block_scale(stream_key, extent, cuts, smallest, high):
    gain = 1.0
    for dim, parts in cuts:
        heights = jax.random.uniform(jax.random.fold_in(jax.random.fold_in(stream_key, 6), dim), (parts,), jnp.float32, smallest / len(cuts), high / len(cuts))
        gain = gain * jnp.repeat(jnp.exp(heights), extent[dim] // parts).reshape((-1,) + (1,) * (len(extent) - 1 - dim))
    return gain


def gaussian(stream_key, extent, deviation, reach, cuts=(), dtype=jnp.bfloat16):
    gain = block_scale(stream_key, extent, cuts, -0.22, 0.18) if cuts else 1.0
    result = jax.random.normal(stream_key, extent, jnp.float32) * deviation * gain
    return jnp.minimum(jnp.maximum(result, -reach), reach).astype(dtype)


def setup_inputs(seed: int = 0) -> dict:
    splits = jax.random.split(jax.random.key(seed), 11)
    tokens = gaussian(splits[0], (TOKENS, D), 1.0, 6.0, ((0, 16),))
    targets = gaussian(splits[1], (TOKENS, D), 1.0, 6.0, ((0, 16),))
    norm_gain = jnp.clip(1.0 + 0.15 * jax.random.normal(splits[2], (D,), jnp.float32), 0.25, 1.75)
    up_frozen = gaussian(splits[3], (D, FF), D ** -0.5, 0.125, ((0, 16), (1, 2)))
    down_frozen = gaussian(splits[4], (FF, D), FF ** -0.5, 0.0625, ((0, 2), (1, 16)))
    up_left = gaussian(splits[5], (RANK, D), (max(D // 49, 1)) ** -0.5, 1.0, (), jnp.float32)
    up_right = gaussian(splits[6], (RANK, FF), 196 ** -0.5, 0.4375, ((1, 2),), jnp.float32)
    down_left = gaussian(splits[7], (RANK, FF), (max(FF // 76, 1)) ** -0.5, 0.625, ((1, 2),), jnp.float32)
    down_right = gaussian(splits[8], (RANK, D), (4 * D) ** -0.5, 0.0625, (), jnp.float32)
    counts = set_ends(jax.random.randint(splits[9], (CLIENTS,), 64, 4097), jax.random.fold_in(splits[9], 1), 64, 4096).astype(jnp.int32)
    return {"tokens": tokens, "targets": targets, "norm_gain": norm_gain, "up_frozen": up_frozen, "down_frozen": down_frozen, "up_left": up_left, "up_right": up_right, "down_left": down_left, "down_right": down_right, "counts": counts}


LEARN_RATE = 0.01
PROX_WEIGHT = 10.0
ADAPTER_SCALING = 0.5
NORM_EPS = 1e-05

def contracted_rows(left, right):
    return lax.dot_general(left, right, (((0,), (0,)), ((), ())), preferred_element_type=jnp.float32)

def contract_columns(left, right):
    return lax.dot_general(left, right, (((1,), (1,)), ((), ())), preferred_element_type=jnp.float32)

def local_train(batch, goal, norm_gain, up_frozen, down_frozen, start):
    wide = batch.astype(jnp.float32)
    scale = lax.rsqrt(lax.optimization_barrier(jnp.mean(wide * wide, axis=1, keepdims=True)) + NORM_EPS)
    normalized_input = (wide * scale * norm_gain).astype(jnp.bfloat16)
    frozen_hidden_rows = jnp.dot(normalized_input, up_frozen, preferred_element_type=jnp.float32)
    params = start
    for local_step in range(STEPS):
        up_left_b = params[0].astype(jnp.bfloat16)
        up_right_batch = params[1].astype(jnp.bfloat16)
        down_left_b = params[2].astype(jnp.bfloat16)
        down_right_batch = params[3].astype(jnp.bfloat16)
        up_low_product = contract_columns(normalized_input, up_left_b).astype(jnp.bfloat16)
        hidden_preactivation = frozen_hidden_rows + ADAPTER_SCALING * jnp.dot(up_low_product, up_right_batch, preferred_element_type=jnp.float32)
        gated_hidden = jax.nn.silu(hidden_preactivation).astype(jnp.bfloat16)
        down_low_product = contract_columns(gated_hidden, down_left_b).astype(jnp.bfloat16)
        layer_output = batch.astype(jnp.float32) + jnp.dot(gated_hidden, down_frozen, preferred_element_type=jnp.float32)
        layer_output = layer_output + ADAPTER_SCALING * jnp.dot(down_low_product, down_right_batch, preferred_element_type=jnp.float32)
        output_gradient = ((layer_output - goal.astype(jnp.float32)) / TOK_CLIENT).astype(jnp.bfloat16)
        down_low_gradient = (ADAPTER_SCALING * contract_columns(output_gradient, down_right_batch)).astype(jnp.bfloat16)
        d_gated = contract_columns(output_gradient, down_frozen) + jnp.dot(down_low_gradient, down_left_b, preferred_element_type=jnp.float32)
        sigmoid_pre = jax.nn.sigmoid(hidden_preactivation)
        hidden_gradient = (d_gated * sigmoid_pre * (1.0 + hidden_preactivation * (1.0 - sigmoid_pre))).astype(jnp.bfloat16)
        up_low_gradient = (ADAPTER_SCALING * contract_columns(hidden_gradient, up_right_batch)).astype(jnp.bfloat16)
        gradient_tree = (contracted_rows(up_low_gradient, normalized_input), ADAPTER_SCALING * contracted_rows(up_low_product, hidden_gradient), contracted_rows(down_low_gradient, gated_hidden), ADAPTER_SCALING * contracted_rows(down_low_product, output_gradient))

        def update(value, grad, anchor):
            return value - LEARN_RATE * (grad + PROX_WEIGHT * (value - anchor))
        params = jax.tree.map(update, params, gradient_tree, start)
    return params

def reference(tokens, targets, norm_gain, up_frozen, down_frozen, up_left, up_right, down_left, down_right, counts):
    token_rows = tokens.reshape(N_CLIENT, TOK_CLIENT, D)
    goal_rows = targets.reshape(N_CLIENT, TOK_CLIENT, D)
    start = (up_left, up_right, down_left, down_right)

    def visit(carry, item):
        batch, goal, weight = item
        final = local_train(batch, goal, norm_gain, up_frozen, down_frozen, start)
        scaled = weight.astype(jnp.float32)

        def accumulate(total, anchor, value):
            return total + scaled * (anchor - value)
        sums = jax.tree.map(accumulate, carry[0], start, final)
        return ((sums, carry[1] + scaled), None)
    zeros = jax.tree.map(jnp.zeros_like, start)
    (sums, total), unused = lax.scan(visit, (zeros, jnp.zeros((), jnp.float32)), (token_rows, goal_rows, counts))
    factor = LEARN_RATE * total
    return (sums[0] / factor, sums[1] / factor, sums[2] / factor, sums[3] / factor)
```

```python
import functools

import jax
import jax.numpy as jnp
from jax import lax
from jax.experimental import pallas as pl
from jax.experimental.pallas import tpu as pltpu
from jax.sharding import PartitionSpec as P

STEPS = 3
LEARN_RATE = 0.01
PROX_WEIGHT = 10.0
ADAPTER_SCALING = 0.5
NORM_EPS = 1e-05
LANES = 128

F32 = jnp.float32
BF16 = jnp.bfloat16


def mm(a, b):
    return lax.dot_general(a, b, (((1,), (0,)), ((), ())), preferred_element_type=F32)


def mmt(a, b):
    return lax.dot_general(a, b, (((1,), (1,)), ((), ())), preferred_element_type=F32)


def update(value, grad, anchor):
    return value - LEARN_RATE * (grad + PROX_WEIGHT * (value - anchor))


def kernel(n, subs, bpa, bpb, tile, groups, up, dn, tokens, targets, gain, ul0h, ur0h, dl0h, dr0h, count,
           res,
           w0, w1, base, dact, gate, act, dpre, ptx, prx, dout, nx, diff,
           dnv, gainv, ul0, ur0, dl0, dr0,
           ul0p, dr0p, ulp, drp, ur, dl, ulb, drb, urb, dlb,
           lut, ldt, dldt, ldm, xtx, xrx, cntb,
           sbuf, abuf, bbuf, cbuf, rbuf,
           up_s, in_s, ring_s, ring_r, sib_s, sib_r, p_s, p_r, x_s, x_r, c_s, c_r,
           ab_s, ab_r, b_s, b_r, g_s, g_r, f_s, f_r):
    R = n // 2
    half_ring = R // 2
    me = lax.axis_index("client")
    tp = lax.axis_index("tp")
    chip = me // 2
    core = me % 2
    sib = chip * 2 + (1 - core)
    ws = (w0, w1)
    rows, ffl = up.shape
    cr = 2 * rows
    half = rows // 2
    piece = half // subs
    tok = tokens.shape[0]
    rank = ul0.shape[0]
    n_tiles = ffl // tile

    low = chip % 2
    pos = jnp.where(low == 0, chip // 2, R - 1 - chip // 2)

    def chip_at(p):
        p = (p + 2 * R) % R
        return jnp.where(p < half_ring, 2 * p, 2 * (R - 1 - p) + 1)

    def slot_of(k, d):
        owner = k // 2
        at = owner // 2 if owner % 2 == 0 else R - 1 - owner // 2
        return (pos - at + R) % R if d == 0 else (at - pos + R) % R

    def lanes_of(k, d):
        return slice(d * rows + k % 2 * half, d * rows + k % 2 * half + half)

    def copy(src, dst, ss, rs, client, t):
        return pltpu.make_async_remote_copy(
            src_ref=src, dst_ref=dst, send_sem=ss, recv_sem=rs,
            device_id={"client": client, "tp": t},
            device_id_type=pl.DeviceIdType.MESH)

    nbr = (chip_at(pos + 1) * 2 + core, chip_at(pos - 1) * 2 + core)
    parts = [(d, u) for u in range(subs) for d in range(2)]

    def place(m, d, s, u, c):
        start = pl.multiple_of(d * rows + c * half + u * piece, piece)
        return ws[m].at[s, pl.ds(start, piece)]

    def ring_copy(m, d, s, u):
        return copy(place(m, d, s, u, core), place(m, d, s + 1, u, core),
                    ring_s.at[m, d, s, u], ring_r.at[m, d, s + 1, u], nbr[d], tp)

    def ring_arrived(m, d, s, u):
        ref = place(m, d, s, u, core)
        copy(ref, ref, ring_s.at[m, d, 0, u], ring_r.at[m, d, s, u], nbr[d], tp).wait_recv()

    def sib_copy(m, d, s, u, c):
        ref = place(m, d, s, u, c)
        return copy(ref, ref, sib_s.at[m, d, s, u], sib_r.at[m, d, s, u], sib, tp)

    def send_own(m):
        for d, u in parts:
            ring_copy(m, d, 0, u).start()
        for d, u in parts:
            sib_copy(m, d, 0, u, core).start()

    def advance(m, s, forward):
        for d, u in parts:
            ring_arrived(m, d, s, u)
            if forward:
                ring_copy(m, d, s, u).start()
            sib_copy(m, d, s, u, core).start()

    def sib_arrived(m, s):
        for d, u in parts:
            sib_copy(m, d, s, u, 1 - core).wait_recv()

    def tiles(fn, init=0):
        return lax.fori_loop(
            0, n_tiles, lambda i, c: fn(pl.ds(pl.multiple_of(i * tile, tile), tile), c), init,
            unroll=UNROLL if n_tiles % UNROLL == 0 else 1)

    def each_slot(fn, lo=0, hi=None):
        hi = R if hi is None else hi
        if R <= 8:
            for s in range(lo, hi):
                fn(s)
        else:
            pl.loop(lo, hi)(fn)

    def slot_sum(fn, init):
        if R <= 8:
            for s in range(R):
                init = init + fn(s)
            return init
        return lax.fori_loop(0, R, lambda s, c: c + fn(s), init)

    width = tokens.shape[1]
    tokv = dpre.at[:, pl.ds(0, width)]
    tgtv = act.at[:, pl.ds(0, width)]
    ups = [pltpu.make_async_copy(up.at[pl.ds(d * half + u * piece, piece)], place(0, d, 0, u, core), up_s.at[d, u])
           for d, u in parts]
    ins = [pltpu.make_async_copy(a, b, in_s.at[i]) for i, (a, b) in enumerate((
        (tokens, tokv), (gain, gainv), (targets, tgtv), (ul0h, ul0), (ur0h, ur0),
        (dl0h, dl0), (dr0h, dr0), (dn, dnv)))]
    for c in ups:
        c.start()

    barrier = pltpu.get_barrier_semaphore()
    for client, t in ((nbr[0], tp), (nbr[1], tp), (sib, tp), (me, 1 - tp)):
        pl.semaphore_signal(barrier, inc=1, device_id={"client": client, "tp": t},
                            device_id_type=pl.DeviceIdType.MESH)
    pl.semaphore_wait(barrier, 4)

    for own in ups:
        own.wait()
    send_own(0)
    for c in ins:
        c.start()

    for c in ins:
        c.wait()
    strip = 64 if tok % 64 == 0 else tok

    @pl.loop(0, tok // strip)
    def _(i):
        here = pl.ds(pl.multiple_of(i * strip, strip), strip)
        wide = tokv[here, :].astype(F32)
        scale = lax.rsqrt(jnp.mean(wide * wide, axis=1, keepdims=True) + NORM_EPS)
        normed = (wide * scale * gainv[...]).astype(BF16)
        gap = wide - tgtv[here, :].astype(F32)
        for k in range(n):
            for d in range(2):
                at = slice(k * rows + d * half, k * rows + d * half + half)
                nx[slot_of(k, d), here, lanes_of(k, d)] = normed[:, at]
                diff[slot_of(k, d), here, lanes_of(k, d)] = gap[:, at]

    for k in range(n):
        for d in range(2):
            at = slice(k * rows + d * half, k * rows + d * half + half)
            for src, first, now in ((ul0, ul0p, ulp), (dr0, dr0p, drp)):
                first[slot_of(k, d), :, lanes_of(k, d)] = src[:, at]
                now[slot_of(k, d), :, lanes_of(k, d)] = src[:, at]
    ur[...] = ur0[...]
    dl[...] = dl0[...]

    def turned(cols, c):
        flat = dnv[cols, :].T
        for d in range(2):
            w1[0, pl.ds(pl.multiple_of(d * rows + core * half, half), half), cols] = flat[d * half:(d + 1) * half]
        return c

    def add_base(s):
        sib_arrived(0, s)

        def body(cols, c):
            base[:, cols] += mm(nx[s], w0[s, :, cols])
            return c
        tiles(body)

    def first_base():
        sib_arrived(0, 0)

        def body(cols, c):
            base[:, cols] = mm(nx[0], w0[0, :, cols])
            return c
        tiles(body)

    def p_copy(s):
        return copy(ptx.at[s], prx.at[s], p_s.at[s], p_r.at[s], me, 1 - tp)

    def forward_piece(s):
        ptx[s] = mmt(act[...], w1[s]).astype(BF16)

    def output_piece(s):
        p_copy(s).wait_recv()
        total = ptx[s].astype(F32) + prx[s].astype(F32)
        out = diff[s] + total + ADAPTER_SCALING * mm(ldm[...], drb[s])
        grad = (out / tok).astype(BF16)
        dout[s] = grad
        dldt[...] += mmt(drb[s], grad)

    def through(s0, g, cols):
        if g == 1:
            return mm(dout[s0], w1[s0, :, cols])
        if cr % LANES:
            return sum(mm(dout[s0 + i], w1[s0 + i, :, cols]) for i in range(g))
        left = jnp.concatenate([dout[s0 + i] for i in range(g)], axis=1)
        return mm(left, w1[pl.ds(s0, g), :, cols].reshape(g * cr, tile))

    def backward(s0, g, first):
        def body(cols, c):
            d = through(s0, g, cols)
            dact[:, cols] = d if first else dact[:, cols] + d
            return c
        tiles(body)

    def x_copy(k):
        return copy(xtx.at[k], xrx.at[k], x_s.at[k], x_r.at[k], me, 1 - tp)

    def begin_step():
        def narrow(s):
            ulb[s] = ulp[s].astype(BF16)
            drb[s] = drp[s].astype(BF16)
        each_slot(narrow)
        urb[...] = ur[...].astype(BF16)
        dlb[...] = dl[...].astype(BF16)
        low_t = slot_sum(lambda s: mmt(ulb[s], nx[s]), jnp.zeros((rank, tok), F32))
        lut[...] = low_t.astype(BF16)
        lu = low_t.T.astype(BF16)

        def body(cols, c):
            pre = base[:, cols] + ADAPTER_SCALING * mm(lu, urb[:, cols])
            t = 0.5 * jnp.tanh(0.5 * pre)
            sig = 0.5 + t
            a = pre * sig
            ab = a.astype(BF16)
            act[:, cols] = ab
            gate[:, cols] = sig + a * (0.5 - t)
            return c + mmt(dlb[:, cols], ab)
        xtx[0] = tiles(body, jnp.zeros((rank, tok), F32))
        x_copy(0).start()
        dldt[...] = jnp.zeros_like(dldt)

    def take_low():
        x_copy(0).wait_recv()
        total = xtx[0] + xrx[0]
        ldt[...] = total.astype(BF16)
        ldm[...] = total.T.astype(BF16)

    def end_step(s0, g):
        dld = ADAPTER_SCALING * dldt[...]
        dld_t = dld.astype(BF16)
        dld_m = dld.T.astype(BF16)

        def body(cols, c):
            d = dact[:, cols] + through(s0, g, cols) + mm(dld_m, dlb[:, cols])
            h = (d * gate[:, cols]).astype(BF16)
            dpre[:, cols] = h
            return c + mmt(urb[:, cols], h)
        xtx[1] = ADAPTER_SCALING * tiles(body, jnp.zeros((rank, tok), F32))
        x_copy(1).start()

        def rest(cols, c):
            ur[:, cols] = update(ur[:, cols], ADAPTER_SCALING * mm(lut[...], dpre[:, cols]), ur0[:, cols])
            dl[:, cols] = update(dl[:, cols], mm(dld_t, act[:, cols]), dl0[:, cols])
            return c
        tiles(rest)

        def right(s):
            drp[s] = update(drp[s], ADAPTER_SCALING * mm(ldt[...], dout[s]), dr0p[s])
        each_slot(right)

    def end_left():
        x_copy(1).wait_recv()
        dlu_t = (xtx[1] + xrx[1]).astype(BF16)

        def left(s):
            ulp[s] = update(ulp[s], mm(dlu_t, nx[s]), ul0p[s])
        each_slot(left)
        x_copy(0).wait_send()
        x_copy(1).wait_send()

        @pl.loop(0, R)
        def _(s):
            p_copy(s).wait_send()

    first_base()

    @pl.loop(1, R - 1)
    def _(s):
        advance(0, s, True)

        @pl.when(s == 1)
        def _():
            tiles(turned)

        @pl.when(s > 1)
        def _():
            add_base(s - 1)
    send_own(1)
    advance(0, R - 1, False)
    if R > 2:
        add_base(R - 2)
    add_base(R - 1)

    weight = count[0].astype(F32)
    cntb[me] = jnp.full(cntb.shape[1:], weight, F32)

    def cnt_copy(k):
        return copy(cntb.at[me], cntb.at[me], c_s.at[k], c_r.at[me], k, tp)

    @pl.loop(1, n)
    def _(i):
        cnt_copy((me + i) % n).start()
    advance(1, 1, R > 2)
    begin_step()
    sib_arrived(1, 0)
    forward_piece(0)
    p_copy(0).start()
    take_low()

    @pl.loop(2, R)
    def _(s):
        @pl.when(s < R - 1)
        def _():
            advance(1, s, True)

        @pl.when(s == R - 1)
        def _():
            advance(1, s, False)
        sib_arrived(1, s - 1)
        forward_piece(s - 1)
        p_copy(s - 1).start()
        output_piece(s - 2)

        @pl.when(s == 2)
        def _():
            backward(0, 1, True)

        @pl.when(s > 2)
        def _():
            backward(s - 2, 1, False)
    sib_arrived(1, R - 1)
    forward_piece(R - 1)
    p_copy(R - 1).start()
    output_piece(R - 2)
    backward(R - 2, 1, False)
    output_piece(R - 1)
    end_step(R - 1, 1)
    end_left()

    def forward_send(s):
        forward_piece(s)
        p_copy(s).start()

    def later_step():
        begin_step()
        each_slot(forward_send)
        take_low()
        s0 = 0
        for g in groups:
            each_slot(output_piece, s0, s0 + g)
            if s0 + g < R:
                backward(s0, g, s0 == 0)
            s0 += g
        end_step(R - groups[-1], groups[-1])

    @pl.loop(1, STEPS - 1)
    def _(t):
        later_step()
        end_left()
    later_step()

    def pack(b, i0, per, change):
        owner, i = divmod(b, per)
        c, k = divmod(owner, R)
        sbuf[c, k, i0 + i] = (weight * change).astype(BF16)

    b = 0
    for value, anchor in ((ur, ur0), (dl, dl0)):
        for at in range(0, ffl, LANES):
            pack(b, 0, bpa, anchor[:, at:at + LANES] - value[:, at:at + LANES])
            b += 1

    def wide_block(anchor, value, at):
        bits = []
        for lo in range(at, at + LANES, half):
            k, d = lo // rows, lo % rows // half
            where = (slot_of(k, d), slice(None), lanes_of(k, d))
            bits.append(anchor[where] - value[where])
        return jnp.concatenate(bits, axis=1)

    d = R * cr
    for at in range(0, d, LANES):
        pack(b, 0, bpa, wide_block(dr0p, drp, at))
        b += 1
    for b in range(b, n * bpa):
        pack(b, 0, bpa, jnp.zeros(sbuf.shape[3:], F32))
    spans = (pl.ds(0, bpa), pl.ds(bpa, bpb))

    def pair(q):
        return copy(sbuf.at[1 - core, :, spans[q]], abuf.at[:, spans[q]], ab_s.at[q], ab_r.at[q], sib, tp)
    pair(0).start()
    end_left()
    b = 0
    for at in range(0, d, LANES):
        pack(b, bpa, bpb, wide_block(ul0p, ulp, at))
        b += 1
    for b in range(b, n * bpb):
        pack(b, bpa, bpb, jnp.zeros(sbuf.shape[3:], F32))
    pair(1).start()

    @pl.loop(1, n)
    def _(i):
        k = (me + i) % n
        copy(cntb.at[k], cntb.at[k], c_s.at[k], c_r.at[k], k, tp).wait_recv()
    total = lax.fori_loop(0, n, lambda k, c: c + cntb[k], jnp.zeros(cntb.shape[1:], F32))
    factor = LEARN_RATE * total[0:1, 0:1]

    def chip_copy(q, k):
        return copy(bbuf.at[k, spans[q]], cbuf.at[chip, spans[q]], b_s.at[q, k], b_r.at[q, chip], k * 2 + core, tp)

    def chip_arrived(q, k):
        copy(bbuf.at[k, spans[q]], cbuf.at[k, spans[q]], b_s.at[q, k], b_r.at[q, k], k * 2 + core, tp).wait_recv()

    def back_copy(q, k):
        ref = rbuf.at[core, chip, spans[q]]
        return copy(ref, ref, g_s.at[q, k], g_r.at[q, chip], k * 2 + core, tp)

    def back_arrived(q, k):
        ref = rbuf.at[core, k, spans[q]]
        copy(ref, ref, g_s.at[q, k], g_r.at[q, k], k * 2 + core, tp).wait_recv()

    def pass_copy(q, c, k):
        ref = rbuf.at[c, k, spans[q]]
        return copy(ref, ref, f_s.at[q, k], f_r.at[q, k], sib, tp)

    for q in range(2):
        pair(q).wait_recv()

        @pl.loop(0, R)
        def _(i):
            k = (chip + 1 + i) % R
            bbuf[k, spans[q]] = (sbuf[core, k, spans[q]].astype(F32) + abuf[k, spans[q]].astype(F32)).astype(BF16)

            @pl.when(i < R - 1)
            def _():
                chip_copy(q, k).start()
        cbuf[chip, spans[q]] = bbuf[chip, spans[q]]
    for q in range(2):
        @pl.loop(1, R)
        def _(i):
            chip_arrived(q, (chip + i) % R)
        s = lax.fori_loop(0, R, lambda k, c: c + cbuf[k, spans[q]].astype(F32),
                          jnp.zeros((spans[q].size,) + cbuf.shape[2:], F32))
        rbuf[core, chip, spans[q]] = (s / factor).astype(BF16)

        @pl.loop(1, R)
        def _(i):
            back_copy(q, (chip + i) % R).start()
        pass_copy(q, core, chip).start()
    for q in range(2):
        @pl.loop(1, R)
        def _(i):
            k = (chip + i) % R
            back_arrived(q, k)
            pass_copy(q, core, k).start()
    for q in range(2):
        @pl.loop(0, R)
        def _(k):
            pass_copy(q, 1 - core, k).wait_recv()
    res[...] = rbuf[...]

    for q in range(2):
        pair(q).wait_send()

        @pl.loop(1, R)
        def _(i):
            k = (chip + i) % R
            chip_copy(q, k).wait_send()
            back_copy(q, k).wait_send()

        @pl.loop(0, R)
        def _(k):
            pass_copy(q, core, k).wait_send()

    @pl.loop(1, n)
    def _(i):
        cnt_copy((me + i) % n).wait_send()
    for m in range(2):
        for d, u in parts:
            @pl.loop(0, R)
            def _(s):
                sib_copy(m, d, s, u, core).wait_send()

            @pl.loop(0, R - 1)
            def _(s):
                ring_copy(m, d, s, u).wait_send()


UNROLL = 7


def spread(n, bpa, bpb, res, oul, our, odl, odr):
    R = n // 2

    def take(b, i0, per, out, at):
        owner, i = divmod(b, per)
        c, k = divmod(owner, R)
        out[:, at:at + LANES] = res[c, k, i0 + i].astype(F32)
    b = 0
    for out in (our, odl, odr):
        for at in range(0, out.shape[1], LANES):
            take(b, 0, bpa, out, at)
            b += 1
    for b, at in enumerate(range(0, oul.shape[1], LANES)):
        take(b, bpa, bpb, oul, at)


def per_device(n, tokens, targets, norm_gain, up_frozen, down_frozen,
               up_left, up_right, down_left, down_right, counts):
    R = n // 2
    tok, d = tokens.shape
    rank = up_left.shape[0]
    rows, ffl = up_frozen.shape
    cr = 2 * rows
    subs = 2 if rows % 64 == 0 else 1
    tile = 512 if ffl % 512 == 0 else 128
    groups, left = [], R
    while left > 1:
        groups.append(min(4, left // 2))
        left -= groups[-1]
    groups.append(1)
    bpa = -(-(2 * ffl + d) // (LANES * n))
    bpb = -(-d // (LANES * n))
    bpd = bpa + bpb
    vm = pl.BlockSpec(memory_space=pltpu.VMEM)
    sm = pl.BlockSpec(memory_space=pltpu.SMEM)
    hbm = pl.BlockSpec(memory_space=pl.ANY)
    V = pltpu.VMEM
    dma = lambda *s: pltpu.SemaphoreType.DMA(s)
    packed = pl.pallas_call(
        functools.partial(kernel, n, subs, bpa, bpb, tile, tuple(groups)),
        out_shape=jax.ShapeDtypeStruct((2, R, bpd, rank, LANES), BF16),
        in_specs=[hbm] * 9 + [sm],
        out_specs=vm,
        scratch_shapes=[
            V((R, cr, ffl), BF16), V((R, cr, ffl), BF16),
            V((tok, ffl), F32), V((tok, ffl), F32), V((tok, ffl), F32),
            V((tok, ffl), BF16), V((tok, ffl), BF16),
            V((R, tok, cr), BF16), V((R, tok, cr), BF16), V((R, tok, cr), BF16),
            V((R, tok, cr), BF16), V((R, tok, cr), F32),
            V((ffl, rows), BF16), V((1, d), F32),
            V((rank, d), F32), V((rank, ffl), F32), V((rank, ffl), F32), V((rank, d), F32),
            V((R, rank, cr), F32), V((R, rank, cr), F32), V((R, rank, cr), F32), V((R, rank, cr), F32),
            V((rank, ffl), F32), V((rank, ffl), F32),
            V((R, rank, cr), BF16), V((R, rank, cr), BF16), V((rank, ffl), BF16), V((rank, ffl), BF16),
            V((rank, tok), BF16), V((rank, tok), BF16), V((rank, tok), F32), V((tok, rank), BF16),
            V((2, rank, tok), F32), V((2, rank, tok), F32), V((n, 8, LANES), F32),
            V((2, R, bpd, rank, LANES), BF16), V((R, bpd, rank, LANES), BF16),
            V((R, bpd, rank, LANES), BF16), V((R, bpd, rank, LANES), BF16),
            V((2, R, bpd, rank, LANES), BF16),
            dma(2, subs), dma(8), dma(2, 2, R, subs), dma(2, 2, R, subs), dma(2, 2, R, subs), dma(2, 2, R, subs),
            dma(R), dma(R), dma(2), dma(2), dma(n), dma(n),
            dma(2), dma(2), dma(2, R), dma(2, R), dma(2, R), dma(2, R), dma(2, R), dma(2, R),
        ],
        compiler_params=pltpu.CompilerParams(
            vmem_limit_bytes=65400 * 1024, has_side_effects=True, collective_id=0),
    )(up_frozen, down_frozen, tokens, targets, norm_gain.reshape(1, d),
      up_left, up_right, down_left, down_right, counts)
    return pl.pallas_call(
        functools.partial(spread, n, bpa, bpb),
        out_shape=[jax.ShapeDtypeStruct(a.shape, F32)
                   for a in (up_left, up_right, down_left, down_right)],
        in_specs=[vm],
        out_specs=[vm] * 4,
    )(packed)


def solution(mesh):
    placed = (
        P("client", None),
        P("client", None),
        P(),
        P("client", "tp"),
        P("tp", "client"),
        P(),
        P(None, "tp"),
        P(None, "tp"),
        P(),
        P("client"),
    )
    return jax.shard_map(
        functools.partial(per_device, mesh.shape["client"]),
        mesh=mesh,
        in_specs=placed,
        out_specs=(P(), P(None, "tp"), P(None, "tp"), P()),
        check_vma=False,
    )
```

```python
import functools

import jax
import jax.numpy as jnp
from jax import lax
from jax.experimental import pallas as pl
from jax.experimental.pallas import tpu as pltpu
from jax.sharding import PartitionSpec as P

STEPS = 3
LEARN_RATE = 0.01
PROX_WEIGHT = 10.0
ADAPTER_SCALING = 0.5
NORM_EPS = 1e-05
LANES = 128

F32 = jnp.float32
BF16 = jnp.bfloat16
UNROLL = 7


def mm(a, b):
    return lax.dot_general(a, b, (((1,), (0,)), ((), ())), preferred_element_type=F32)


def mmt(a, b):
    return lax.dot_general(a, b, (((1,), (1,)), ((), ())), preferred_element_type=F32)


def update(value, grad, anchor):
    return value - LEARN_RATE * (grad + PROX_WEIGHT * (value - anchor))


def kernel(n, subs, bpa, bpb, tile, groups, up, dn, tokens, targets, gain, ul0h, ur0h, dl0h, dr0h, count,
           res,
           w0, w1, base, dact, gate, act, dpre, ptx, prx, dout, nx, diff,
           dnv, gainv, ul0, ur0, dl0, dr0,
           ul0p, dr0p, ulp, drp, ur, dl, ulb, drb, urb, dlb,
           lut, ldt, dldt, ldm, xtx, xrx, cntb,
           sbuf, abuf, bbuf, cbuf, rbuf,
           up_s, in_s, ring_s, ring_r, sib_s, sib_r, p_s, p_r, x_s, x_r, c_s, c_r,
           ab_s, ab_r, b_s, b_r, g_s, g_r, f_s, f_r, turn):
    R = n // 2
    half_ring = R // 2
    me = lax.axis_index("client")
    tp = lax.axis_index("tp")
    chip = me // 2
    core = me % 2
    sib = chip * 2 + (1 - core)
    ws = (w0, w1)
    rows, ffl = up.shape
    cr = 2 * rows
    half = rows // 2
    piece = half // subs
    tok = tokens.shape[0]
    rank = ul0.shape[0]
    n_tiles = ffl // tile

    low = chip % 2
    pos = jnp.where(low == 0, chip // 2, R - 1 - chip // 2)

    def chip_at(p):
        p = (p + 2 * R) % R
        return jnp.where(p < half_ring, 2 * p, 2 * (R - 1 - p) + 1)

    def slot_of(k, d):
        owner = k // 2
        at = owner // 2 if owner % 2 == 0 else R - 1 - owner // 2
        return (pos - at + R) % R if d == 0 else (at - pos + R) % R

    def lanes_of(k, d):
        return slice(d * rows + k % 2 * half, d * rows + k % 2 * half + half)

    def copy(src, dst, ss, rs, client, t):
        return pltpu.make_async_remote_copy(
            src_ref=src, dst_ref=dst, send_sem=ss, recv_sem=rs,
            device_id={"client": client, "tp": t},
            device_id_type=pl.DeviceIdType.MESH)

    nbr = (chip_at(pos + 1) * 2 + core, chip_at(pos - 1) * 2 + core)
    parts = [(d, u) for u in range(subs) for d in range(2)]

    def place(m, d, s, u, c):
        start = pl.multiple_of(d * rows + c * half + u * piece, piece)
        return ws[m].at[s, pl.ds(start, piece)]

    def ring_copy(m, d, s, u):
        return copy(place(m, d, s, u, core), place(m, d, s + 1, u, core),
                    ring_s.at[m, d, s, u], ring_r.at[m, d, s + 1, u], nbr[d], tp)

    def ring_arrived(m, d, s, u):
        ref = place(m, d, s, u, core)
        copy(ref, ref, ring_s.at[m, d, 0, u], ring_r.at[m, d, s, u], nbr[d], tp).wait_recv()

    def sib_copy(m, d, s, u, c):
        ref = place(m, d, s, u, c)
        return copy(ref, ref, sib_s.at[m, d, s, u], sib_r.at[m, d, s, u], sib, tp)

    def send_own(m):
        for d, u in parts:
            ring_copy(m, d, 0, u).start()
        for d, u in parts:
            sib_copy(m, d, 0, u, core).start()

    def advance(m, s, forward):
        for d, u in parts:
            ring_arrived(m, d, s, u)
            if forward:
                ring_copy(m, d, s, u).start()
            sib_copy(m, d, s, u, core).start()

    def sib_arrived(m, s):
        for d, u in parts:
            sib_copy(m, d, s, u, 1 - core).wait_recv()

    def tiles(fn, init=0, unroll=1):
        return lax.fori_loop(
            0, n_tiles, lambda i, c: fn(pl.ds(pl.multiple_of(i * tile, tile), tile), c), init,
            unroll=unroll)

    def each_slot(fn, lo=0, hi=None):
        hi = R if hi is None else hi
        if R <= 8:
            for s in range(lo, hi):
                fn(s)
        else:
            pl.loop(lo, hi)(fn)

    def slot_sum(fn, init):
        if R <= 8:
            for s in range(R):
                init = init + fn(s)
            return init
        return lax.fori_loop(0, R, lambda s, c: c + fn(s), init)

    width = tokens.shape[1]
    tokv = dpre.at[:, pl.ds(0, width)]
    tgtv = act.at[:, pl.ds(0, width)]
    ups = [pltpu.make_async_copy(up.at[pl.ds(d * half + u * piece, piece)], place(0, d, 0, u, core), up_s.at[d, u])
           for d, u in parts]
    ins = [pltpu.make_async_copy(a, b, in_s.at[i]) for i, (a, b) in enumerate((
        (tokens, tokv), (gain, gainv), (targets, tgtv), (ul0h, ul0), (ur0h, ur0),
        (dl0h, dl0), (dr0h, dr0), (dn, dnv)))]
    for c in ups:
        c.start()

    barrier = pltpu.get_barrier_semaphore()
    for client, t in ((nbr[0], tp), (nbr[1], tp), (sib, tp), (me, 1 - tp)):
        pl.semaphore_signal(barrier, inc=1, device_id={"client": client, "tp": t},
                            device_id_type=pl.DeviceIdType.MESH)
    pl.semaphore_wait(barrier, 4)

    for own in ups:
        own.wait()
    send_own(0)
    for c in ins:
        c.start()

    for c in ins:
        c.wait()
    strip = 64 if tok % 64 == 0 else tok

    @pl.loop(0, tok // strip)
    def _(i):
        here = pl.ds(pl.multiple_of(i * strip, strip), strip)
        wide = tokv[here, :].astype(F32)
        scale = lax.rsqrt(jnp.mean(wide * wide, axis=1, keepdims=True) + NORM_EPS)
        normed = (wide * scale * gainv[...]).astype(BF16)
        gap = wide - tgtv[here, :].astype(F32)
        for k in range(n):
            for d in range(2):
                at = slice(k * rows + d * half, k * rows + d * half + half)
                nx[slot_of(k, d), here, lanes_of(k, d)] = normed[:, at]
                diff[slot_of(k, d), here, lanes_of(k, d)] = gap[:, at]

    for k in range(n):
        for d in range(2):
            at = slice(k * rows + d * half, k * rows + d * half + half)
            for src, first in ((ul0, ul0p), (dr0, dr0p)):
                first[slot_of(k, d), :, lanes_of(k, d)] = src[:, at]
    for first, now, short in ((ul0p, ulp, ulb), (dr0p, drp, drb), (ur0, ur, urb), (dl0, dl, dlb)):
        now[...] = first[...]
        short[...] = first[...].astype(BF16)

    def turned(cols, c):
        flat = dnv[cols, :].T
        for d in range(2):
            w1[0, pl.ds(pl.multiple_of(d * rows + core * half, half), half), cols] = flat[d * half:(d + 1) * half]
        return c

    def add_base(s):
        sib_arrived(0, s)

        def body(cols, c):
            base[:, cols] += mm(nx[s], w0[s, :, cols])
            return c
        tiles(body)

    def first_base():
        sib_arrived(0, 0)

        def body(cols, c):
            base[:, cols] = mm(nx[0], w0[0, :, cols])
            return c
        tiles(body)

    def p_copy(s):
        return copy(ptx.at[s], prx.at[s], p_s.at[s], p_r.at[s], me, 1 - tp)

    def forward_piece(s):
        ptx[s] = mmt(act[...], w1[s]).astype(BF16)

    def output_piece(s):
        p_copy(s).wait_recv()
        total = ptx[s].astype(F32) + prx[s].astype(F32)
        out = diff[s] + total + ADAPTER_SCALING * mm(ldm[...], drb[s])
        grad = (out / tok).astype(BF16)
        dout[s] = grad
        dldt[...] += mmt(drb[s], grad)

    def through(s0, g, cols):
        if g == 1:
            return mm(dout[s0], w1[s0, :, cols])
        if cr % LANES:
            return sum(mm(dout[s0 + i], w1[s0 + i, :, cols]) for i in range(g))
        left = jnp.concatenate([dout[s0 + i] for i in range(g)], axis=1)
        return mm(left, w1[pl.ds(s0, g), :, cols].reshape(g * cr, tile))

    def backward(s0, g, first):
        def body(cols, c):
            d = through(s0, g, cols)
            dact[:, cols] = d if first else dact[:, cols] + d
            return c
        tiles(body, 0, UNROLL)

    def x_copy(k):
        return copy(xtx.at[k], xrx.at[k], x_s.at[k], x_r.at[k], me, 1 - tp)

    def begin_step():
        low_t = slot_sum(lambda s: mmt(ulb[s], nx[s]), jnp.zeros((rank, tok), F32))
        lut[...] = low_t.astype(BF16)
        lu = low_t.T.astype(BF16)

        def body(cols, c):
            pre = base[:, cols] + ADAPTER_SCALING * mm(lu, urb[:, cols])
            t = 0.5 * jnp.tanh(0.5 * pre)
            sig = 0.5 + t
            a = pre * sig
            ab = a.astype(BF16)
            act[:, cols] = ab
            gate[:, cols] = sig + a * (0.5 - t)
            return c + mmt(dlb[:, cols], ab)
        xtx[0] = tiles(body, jnp.zeros((rank, tok), F32), UNROLL)
        x_copy(0).start()
        dldt[...] = jnp.zeros_like(dldt)

    def take_low():
        x_copy(0).wait_recv()
        total = xtx[0] + xrx[0]
        ldt[...] = total.astype(BF16)
        ldm[...] = total.T.astype(BF16)

    def end_step(s0, g):
        dld = ADAPTER_SCALING * dldt[...]
        dld_t = dld.astype(BF16)
        dld_m = dld.T.astype(BF16)

        def body(cols, c):
            d = dact[:, cols] + through(s0, g, cols) + mm(dld_m, dlb[:, cols])
            h = (d * gate[:, cols]).astype(BF16)
            dpre[:, cols] = h
            return c + mmt(urb[:, cols], h)
        xtx[1] = ADAPTER_SCALING * tiles(body, jnp.zeros((rank, tok), F32), UNROLL)
        x_copy(1).start()

        def rest(cols, c):
            new = update(ur[:, cols], ADAPTER_SCALING * mm(lut[...], dpre[:, cols]), ur0[:, cols])
            ur[:, cols] = new
            urb[:, cols] = new.astype(BF16)
            new = update(dl[:, cols], mm(dld_t, act[:, cols]), dl0[:, cols])
            dl[:, cols] = new
            dlb[:, cols] = new.astype(BF16)
            return c
        tiles(rest, 0, UNROLL)

        def right(s):
            new = update(drp[s], ADAPTER_SCALING * mm(ldt[...], dout[s]), dr0p[s])
            drp[s] = new
            drb[s] = new.astype(BF16)
        each_slot(right)

    def end_left():
        x_copy(1).wait_recv()
        dlu_t = (xtx[1] + xrx[1]).astype(BF16)

        def left(s):
            new = update(ulp[s], mm(dlu_t, nx[s]), ul0p[s])
            ulp[s] = new
            ulb[s] = new.astype(BF16)
        each_slot(left)
        x_copy(0).wait_send()
        x_copy(1).wait_send()

        @pl.loop(0, R)
        def _(s):
            p_copy(s).wait_send()

    first_base()

    @pl.loop(1, R - 1)
    def _(s):
        advance(0, s, True)

        @pl.when(s == 1)
        def _():
            tiles(turned)

        @pl.when(s > 1)
        def _():
            add_base(s - 1)
    send_own(1)
    advance(0, R - 1, False)
    if R > 2:
        add_base(R - 2)
    add_base(R - 1)

    weight = count[0].astype(F32)
    cntb[me] = jnp.full(cntb.shape[1:], weight, F32)

    def cnt_copy(k):
        return copy(cntb.at[me], cntb.at[me], c_s.at[k], c_r.at[me], k, tp)

    @pl.loop(1, n)
    def _(i):
        cnt_copy((me + i) % n).start()
    advance(1, 1, R > 2)
    def pack(b, i0, per, change):
        owner, i = divmod(b, per)
        c, k = divmod(owner, R)
        sbuf[c, k, i0 + i] = (weight * change).astype(BF16)

    def wide_block(anchor, value, at):
        bits = []
        for lo in range(at, at + LANES, half):
            k, d = lo // rows, lo % rows // half
            where = (slot_of(k, d), slice(None), lanes_of(k, d))
            bits.append(anchor[where] - value[where])
        return jnp.concatenate(bits, axis=1)

    d = R * cr
    spans = (pl.ds(0, bpa), pl.ds(bpa, bpb))

    def pair(q):
        return copy(sbuf.at[1 - core, :, spans[q]], abuf.at[:, spans[q]], ab_s.at[q], ab_r.at[q], sib, tp)
    def chip_copy(q, k):
        return copy(bbuf.at[k, spans[q]], cbuf.at[chip, spans[q]], b_s.at[q, k], b_r.at[q, chip], k * 2 + core, tp)

    def chip_arrived(q, k):
        copy(bbuf.at[k, spans[q]], cbuf.at[k, spans[q]], b_s.at[q, k], b_r.at[q, k], k * 2 + core, tp).wait_recv()

    def back_copy(q, k):
        ref = rbuf.at[core, chip, spans[q]]
        return copy(ref, ref, g_s.at[q, k], g_r.at[q, chip], k * 2 + core, tp)

    def back_arrived(q, k):
        ref = rbuf.at[core, k, spans[q]]
        copy(ref, ref, g_s.at[q, k], g_r.at[q, k], k * 2 + core, tp).wait_recv()

    def pass_copy(q, c, k):
        ref = rbuf.at[c, k, spans[q]]
        return copy(ref, ref, f_s.at[q, k], f_r.at[q, k], sib, tp)

    def to_chips(q):
        pair(q).wait_recv()

        @pl.loop(0, R)
        def _(i):
            k = (chip + 1 + i) % R
            bbuf[k, spans[q]] = (sbuf[core, k, spans[q]].astype(F32) + abuf[k, spans[q]].astype(F32)).astype(BF16)

            @pl.when(i < R - 1)
            def _():
                chip_copy(q, k).start()
        cbuf[chip, spans[q]] = bbuf[chip, spans[q]]

    def last_sums():
        b = 0
        for value, anchor in ((ur, ur0), (dl, dl0)):
            for at in range(0, ffl, LANES):
                pack(b, 0, bpa, anchor[:, at:at + LANES] - value[:, at:at + LANES])
                b += 1

        for at in range(0, d, LANES):
            pack(b, 0, bpa, wide_block(dr0p, drp, at))
            b += 1
        for b in range(b, n * bpa):
            pack(b, 0, bpa, jnp.zeros(sbuf.shape[3:], F32))
        pair(0).start()

        to_chips(0)


    def gather_middle():
        sib_arrived(1, 0)
        forward_piece(0)
        p_copy(0).start()
        take_low()

        @pl.loop(2, R + 1)
        def _(s):
            @pl.when(s < R - 1)
            def _():
                advance(1, s, True)

            @pl.when(s == R - 1)
            def _():
                advance(1, s, False)
            sib_arrived(1, s - 1)
            forward_piece(s - 1)
            p_copy(s - 1).start()
            output_piece(s - 2)

            @pl.when(s == 2)
            def _():
                backward(0, 1, True)

            @pl.when(s > 2)
            def _():
                backward(s - 2, 1, False)
        output_piece(R - 1)

    def middle(t):
        held = t == 1

        @pl.loop(0, R)
        def _(s):
            forward_piece(s)

            @pl.when(jnp.logical_not(held & (core == 1)))
            def _():
                p_copy(s).start()

        @pl.when(held & (core == 1))
        def _():
            pl.semaphore_wait(turn, 1)

            @pl.loop(0, R)
            def _(s):
                p_copy(s).start()
        take_low()
        s0 = 0
        for g in groups:
            @pl.loop(s0, s0 + g)
            def _(s):
                output_piece(s)
            if s0 + g < R:
                backward(s0, g, s0 == 0)
            if s0 == 0:
                @pl.when(held & (core == 0))
                def _():
                    pl.semaphore_signal(turn, inc=1, device_id={"client": sib, "tp": tp},
                                        device_id_type=pl.DeviceIdType.MESH)
            s0 += g

    def step(t):
        begin_step()
        pl.when(t == 0)(gather_middle)
        pl.when(t > 0)(functools.partial(middle, t))
        end_step(R - 1, 1)

    @pl.loop(0, STEPS)
    def _(t):
        step(t)
        pl.when(t == STEPS - 1)(last_sums)
        end_left()

    b = 0
    for at in range(0, d, LANES):
        pack(b, bpa, bpb, wide_block(ul0p, ulp, at))
        b += 1
    for b in range(b, n * bpb):
        pack(b, bpa, bpb, jnp.zeros(sbuf.shape[3:], F32))
    pair(1).start()

    @pl.loop(1, n)
    def _(i):
        k = (me + i) % n
        copy(cntb.at[k], cntb.at[k], c_s.at[k], c_r.at[k], k, tp).wait_recv()
    total = lax.fori_loop(0, n, lambda k, c: c + cntb[k], jnp.zeros(cntb.shape[1:], F32))
    factor = LEARN_RATE * total[0:1, 0:1]
    to_chips(1)
    for q in range(2):
        @pl.loop(1, R)
        def _(i):
            chip_arrived(q, (chip + i) % R)
        s = lax.fori_loop(0, R, lambda k, c: c + cbuf[k, spans[q]].astype(F32),
                          jnp.zeros((spans[q].size,) + cbuf.shape[2:], F32))
        rbuf[core, chip, spans[q]] = (s / factor).astype(BF16)

        @pl.loop(1, R)
        def _(i):
            back_copy(q, (chip + i) % R).start()
        pass_copy(q, core, chip).start()
    for q in range(2):
        @pl.loop(1, R)
        def _(i):
            k = (chip + i) % R
            back_arrived(q, k)
            pass_copy(q, core, k).start()
    for q in range(2):
        @pl.loop(0, R)
        def _(k):
            pass_copy(q, 1 - core, k).wait_recv()
    res[...] = rbuf[...]

    for q in range(2):
        pair(q).wait_send()

        @pl.loop(1, R)
        def _(i):
            k = (chip + i) % R
            chip_copy(q, k).wait_send()
            back_copy(q, k).wait_send()

        @pl.loop(0, R)
        def _(k):
            pass_copy(q, core, k).wait_send()

    @pl.loop(1, n)
    def _(i):
        cnt_copy((me + i) % n).wait_send()
    for m in range(2):
        for d, u in parts:
            @pl.loop(0, R)
            def _(s):
                sib_copy(m, d, s, u, core).wait_send()

            @pl.loop(0, R - 1)
            def _(s):
                ring_copy(m, d, s, u).wait_send()


def spread(n, bpa, bpb, res, oul, our, odl, odr):
    R = n // 2

    def take(b, i0, per, out, at):
        owner, i = divmod(b, per)
        c, k = divmod(owner, R)
        out[:, at:at + LANES] = res[c, k, i0 + i].astype(F32)
    b = 0
    for out in (our, odl, odr):
        for at in range(0, out.shape[1], LANES):
            take(b, 0, bpa, out, at)
            b += 1
    for b, at in enumerate(range(0, oul.shape[1], LANES)):
        take(b, bpa, bpb, oul, at)


def per_device(n, tokens, targets, norm_gain, up_frozen, down_frozen,
               up_left, up_right, down_left, down_right, counts):
    R = n // 2
    tok, d = tokens.shape
    rank = up_left.shape[0]
    rows, ffl = up_frozen.shape
    cr = 2 * rows
    subs = 2 if rows % 64 == 0 else 1
    tile = 512 if ffl % 512 == 0 else 128
    groups, left = [], R
    while left > 1:
        groups.append(min(4, left // 2))
        left -= groups[-1]
    groups.append(1)
    bpa = -(-(2 * ffl + d) // (LANES * n))
    bpb = -(-d // (LANES * n))
    bpd = bpa + bpb
    vm = pl.BlockSpec(memory_space=pltpu.VMEM)
    sm = pl.BlockSpec(memory_space=pltpu.SMEM)
    hbm = pl.BlockSpec(memory_space=pl.ANY)
    V = pltpu.VMEM
    dma = lambda *s: pltpu.SemaphoreType.DMA(s)
    packed = pl.pallas_call(
        functools.partial(kernel, n, subs, bpa, bpb, tile, tuple(groups)),
        out_shape=jax.ShapeDtypeStruct((2, R, bpd, rank, LANES), BF16),
        in_specs=[hbm] * 9 + [sm],
        out_specs=vm,
        scratch_shapes=[
            V((R, cr, ffl), BF16), V((R, cr, ffl), BF16),
            V((tok, ffl), F32), V((tok, ffl), F32), V((tok, ffl), F32),
            V((tok, ffl), BF16), V((tok, ffl), BF16),
            V((R, tok, cr), BF16), V((R, tok, cr), BF16), V((R, tok, cr), BF16),
            V((R, tok, cr), BF16), V((R, tok, cr), F32),
            V((ffl, rows), BF16), V((1, d), F32),
            V((rank, d), F32), V((rank, ffl), F32), V((rank, ffl), F32), V((rank, d), F32),
            V((R, rank, cr), F32), V((R, rank, cr), F32), V((R, rank, cr), F32), V((R, rank, cr), F32),
            V((rank, ffl), F32), V((rank, ffl), F32),
            V((R, rank, cr), BF16), V((R, rank, cr), BF16), V((rank, ffl), BF16), V((rank, ffl), BF16),
            V((rank, tok), BF16), V((rank, tok), BF16), V((rank, tok), F32), V((tok, rank), BF16),
            V((2, rank, tok), F32), V((2, rank, tok), F32), V((n, 8, LANES), F32),
            V((2, R, bpd, rank, LANES), BF16), V((R, bpd, rank, LANES), BF16),
            V((R, bpd, rank, LANES), BF16), V((R, bpd, rank, LANES), BF16),
            V((2, R, bpd, rank, LANES), BF16),
            dma(2, subs), dma(8), dma(2, 2, R, subs), dma(2, 2, R, subs), dma(2, 2, R, subs), dma(2, 2, R, subs),
            dma(R), dma(R), dma(2), dma(2), dma(n), dma(n),
            dma(2), dma(2), dma(2, R), dma(2, R), dma(2, R), dma(2, R), dma(2, R), dma(2, R),
            pltpu.SemaphoreType.REGULAR,
        ],
        compiler_params=pltpu.CompilerParams(
            vmem_limit_bytes=65400 * 1024, has_side_effects=True, collective_id=0),
    )(up_frozen, down_frozen, tokens, targets, norm_gain.reshape(1, d),
      up_left, up_right, down_left, down_right, counts)
    return pl.pallas_call(
        functools.partial(spread, n, bpa, bpb),
        out_shape=[jax.ShapeDtypeStruct(a.shape, F32)
                   for a in (up_left, up_right, down_left, down_right)],
        in_specs=[vm],
        out_specs=[vm] * 4,
    )(packed)


def solution(mesh):
    placed = (
        P("client", None),
        P("client", None),
        P(),
        P("client", "tp"),
        P("tp", "client"),
        P(),
        P(None, "tp"),
        P(None, "tp"),
        P(),
        P("client"),
    )
    return jax.shard_map(
        functools.partial(per_device, mesh.shape["client"]),
        mesh=mesh,
        in_specs=placed,
        out_specs=(P(), P(None, "tp"), P(None, "tp"), P()),
        check_vma=False,
    )
```

```python
import functools

import jax
import jax.numpy as jnp
from jax import lax
from jax.experimental import pallas as pl
from jax.experimental.pallas import tpu as pltpu
from jax.sharding import PartitionSpec as P

STEPS = 3
LEARN_RATE = 0.01
PROX_WEIGHT = 10.0
ADAPTER_SCALING = 0.5
NORM_EPS = 1e-05
LANES = 128

F32 = jnp.float32
BF16 = jnp.bfloat16
UNROLL = 7


def mm(a, b):
    return lax.dot_general(a, b, (((1,), (0,)), ((), ())), preferred_element_type=F32)


def mmt(a, b):
    return lax.dot_general(a, b, (((1,), (1,)), ((), ())), preferred_element_type=F32)


def update(value, grad, anchor):
    return value - LEARN_RATE * (grad + PROX_WEIGHT * (value - anchor))


def kernel(n, subs, bpa, bpb, tile, groups, up, dn, tokens, targets, gain, ul0h, ur0h, dl0h, dr0h, count,
           res,
           w0, w1, base, dact, gate, act, dpre, ptx, prx, dout, nx, diff,
           dnv, gainv, ul0, ur0, dl0, dr0,
           ul0p, dr0p, ulp, drp, ur, dl, ulb, drb, urb, dlb,
           lut, ldt, dldt, ldm, xtx, xrx, cntb,
           sbuf, abuf, bbuf, cbuf, rbuf,
           up_s, in_s, ring_s, ring_r, sib_s, sib_r, p_s, p_r, x_s, x_r, c_s, c_r,
           ab_s, ab_r, b_s, b_r, g_s, g_r, f_s, f_r, turn):
    R = n // 2
    half_ring = R // 2
    me = lax.axis_index("client")
    tp = lax.axis_index("tp")
    chip = me // 2
    core = me % 2
    sib = chip * 2 + (1 - core)
    ws = (w0, w1)
    rows, ffl = up.shape
    cr = 2 * rows
    half = rows // 2
    piece = half // subs
    tok = tokens.shape[0]
    rank = ul0.shape[0]
    n_tiles = ffl // tile

    low = chip % 2
    pos = jnp.where(low == 0, chip // 2, R - 1 - chip // 2)

    def chip_at(p):
        p = (p + 2 * R) % R
        return jnp.where(p < half_ring, 2 * p, 2 * (R - 1 - p) + 1)

    def slot_of(k, d):
        owner = k // 2
        at = owner // 2 if owner % 2 == 0 else R - 1 - owner // 2
        return (pos - at + R) % R if d == 0 else (at - pos + R) % R

    def lanes_of(k, d):
        return slice(d * rows + k % 2 * half, d * rows + k % 2 * half + half)

    def copy(src, dst, ss, rs, client, t):
        return pltpu.make_async_remote_copy(
            src_ref=src, dst_ref=dst, send_sem=ss, recv_sem=rs,
            device_id={"client": client, "tp": t},
            device_id_type=pl.DeviceIdType.MESH)

    nbr = (chip_at(pos + 1) * 2 + core, chip_at(pos - 1) * 2 + core)
    parts = [(d, u) for u in range(subs) for d in range(2)]

    def place(m, d, s, u, c):
        start = pl.multiple_of(d * rows + c * half + u * piece, piece)
        return ws[m].at[s, pl.ds(start, piece)]

    def ring_copy(m, d, s, u):
        return copy(place(m, d, s, u, core), place(m, d, s + 1, u, core),
                    ring_s.at[m, d, s, u], ring_r.at[m, d, s + 1, u], nbr[d], tp)

    def ring_arrived(m, d, s, u):
        ref = place(m, d, s, u, core)
        copy(ref, ref, ring_s.at[m, d, 0, u], ring_r.at[m, d, s, u], nbr[d], tp).wait_recv()

    def sib_copy(m, d, s, u, c):
        ref = place(m, d, s, u, c)
        return copy(ref, ref, sib_s.at[m, d, s, u], sib_r.at[m, d, s, u], sib, tp)

    def send_own(m):
        for d, u in parts:
            ring_copy(m, d, 0, u).start()
        for d, u in parts:
            sib_copy(m, d, 0, u, core).start()

    def advance(m, s, forward):
        for d, u in parts:
            ring_arrived(m, d, s, u)
            if forward:
                ring_copy(m, d, s, u).start()
            sib_copy(m, d, s, u, core).start()

    def sib_arrived(m, s):
        for d, u in parts:
            sib_copy(m, d, s, u, 1 - core).wait_recv()

    def tiles(fn, init=0, unroll=1):
        return lax.fori_loop(
            0, n_tiles, lambda i, c: fn(pl.ds(pl.multiple_of(i * tile, tile), tile), c), init,
            unroll=unroll)

    def each_slot(fn, lo=0, hi=None):
        hi = R if hi is None else hi
        if R <= 8:
            for s in range(lo, hi):
                fn(s)
        else:
            pl.loop(lo, hi)(fn)

    def slot_sum(fn, init):
        if R <= 8:
            for s in range(R):
                init = init + fn(s)
            return init
        return lax.fori_loop(0, R, lambda s, c: c + fn(s), init)

    width = tokens.shape[1]
    tokv = dpre.at[:, pl.ds(0, width)]
    tgtv = act.at[:, pl.ds(0, width)]
    ups = [pltpu.make_async_copy(up.at[pl.ds(d * half + u * piece, piece)], place(0, d, 0, u, core), up_s.at[d, u])
           for d, u in parts]
    ins = [pltpu.make_async_copy(a, b, in_s.at[i]) for i, (a, b) in enumerate((
        (tokens, tokv), (gain, gainv), (targets, tgtv), (ul0h, ul0), (ur0h, ur0),
        (dl0h, dl0), (dr0h, dr0), (dn, dnv)))]
    for c in ups:
        c.start()

    barrier = pltpu.get_barrier_semaphore()
    for client, t in ((nbr[0], tp), (nbr[1], tp), (sib, tp), (me, 1 - tp)):
        pl.semaphore_signal(barrier, inc=1, device_id={"client": client, "tp": t},
                            device_id_type=pl.DeviceIdType.MESH)
    pl.semaphore_wait(barrier, 4)

    for own, (d, u) in zip(ups, parts):
        own.wait()
        ring_copy(0, d, 0, u).start()
    for d, u in parts:
        sib_copy(0, d, 0, u, core).start()
    for c in ins:
        c.start()

    for c in ins:
        c.wait()
    strip = 64 if tok % 64 == 0 else tok

    @pl.loop(0, tok // strip)
    def _(i):
        here = pl.ds(pl.multiple_of(i * strip, strip), strip)
        wide = tokv[here, :].astype(F32)
        scale = lax.rsqrt(jnp.mean(wide * wide, axis=1, keepdims=True) + NORM_EPS)
        normed = (wide * scale * gainv[...]).astype(BF16)
        gap = wide - tgtv[here, :].astype(F32)
        for k in range(n):
            for d in range(2):
                at = slice(k * rows + d * half, k * rows + d * half + half)
                nx[slot_of(k, d), here, lanes_of(k, d)] = normed[:, at]
                diff[slot_of(k, d), here, lanes_of(k, d)] = gap[:, at]

    for k in range(n):
        for d in range(2):
            at = slice(k * rows + d * half, k * rows + d * half + half)
            for src, first in ((ul0, ul0p), (dr0, dr0p)):
                first[slot_of(k, d), :, lanes_of(k, d)] = src[:, at]
    for first, now, short in ((ul0p, ulp, ulb), (dr0p, drp, drb), (ur0, ur, urb), (dl0, dl, dlb)):
        now[...] = first[...]
        short[...] = first[...].astype(BF16)

    def turned(cols, c):
        flat = dnv[cols, :].T
        for d in range(2):
            w1[0, pl.ds(pl.multiple_of(d * rows + core * half, half), half), cols] = flat[d * half:(d + 1) * half]
        return c

    def add_base(s):
        sib_arrived(0, s)

        def body(cols, c):
            base[:, cols] += mm(nx[s], w0[s, :, cols])
            return c
        tiles(body)

    def first_base():
        sib_arrived(0, 0)

        def body(cols, c):
            base[:, cols] = mm(nx[0], w0[0, :, cols])
            return c
        tiles(body)

    def p_copy(s):
        return copy(ptx.at[s], prx.at[s], p_s.at[s], p_r.at[s], me, 1 - tp)

    def forward_piece(s):
        ptx[s] = mmt(act[...], w1[s]).astype(BF16)

    def output_piece(s):
        p_copy(s).wait_recv()
        total = ptx[s].astype(F32) + prx[s].astype(F32)
        out = diff[s] + total + ADAPTER_SCALING * mm(ldm[...], drb[s])
        grad = (out / tok).astype(BF16)
        dout[s] = grad
        dldt[...] += mmt(drb[s], grad)

    def through(s0, g, cols):
        if g == 1:
            return mm(dout[s0], w1[s0, :, cols])
        if cr % LANES:
            return sum(mm(dout[s0 + i], w1[s0 + i, :, cols]) for i in range(g))
        left = jnp.concatenate([dout[s0 + i] for i in range(g)], axis=1)
        return mm(left, w1[pl.ds(s0, g), :, cols].reshape(g * cr, tile))

    def backward(s0, g, first):
        def body(cols, c):
            d = through(s0, g, cols)
            dact[:, cols] = d if first else dact[:, cols] + d
            return c
        tiles(body, 0, UNROLL)

    def x_copy(k):
        return copy(xtx.at[k], xrx.at[k], x_s.at[k], x_r.at[k], me, 1 - tp)

    def begin_step():
        low_t = slot_sum(lambda s: mmt(ulb[s], nx[s]), jnp.zeros((rank, tok), F32))
        lut[...] = low_t.astype(BF16)
        lu = low_t.T.astype(BF16)

        def body(cols, c):
            pre = base[:, cols] + ADAPTER_SCALING * mm(lu, urb[:, cols])
            t = 0.5 * jnp.tanh(0.5 * pre)
            sig = 0.5 + t
            a = pre * sig
            ab = a.astype(BF16)
            act[:, cols] = ab
            gate[:, cols] = sig + a * (0.5 - t)
            return c + mmt(dlb[:, cols], ab)
        xtx[0] = tiles(body, jnp.zeros((rank, tok), F32), UNROLL)
        x_copy(0).start()
        dldt[...] = jnp.zeros_like(dldt)

    def take_low():
        x_copy(0).wait_recv()
        total = xtx[0] + xrx[0]
        ldt[...] = total.astype(BF16)
        ldm[...] = total.T.astype(BF16)

    def end_step(s0, g):
        dld = ADAPTER_SCALING * dldt[...]
        dld_t = dld.astype(BF16)
        dld_m = dld.T.astype(BF16)

        def body(cols, c):
            d = dact[:, cols] + through(s0, g, cols) + mm(dld_m, dlb[:, cols])
            h = (d * gate[:, cols]).astype(BF16)
            dpre[:, cols] = h
            return c + mmt(urb[:, cols], h)
        xtx[1] = ADAPTER_SCALING * tiles(body, jnp.zeros((rank, tok), F32), UNROLL)
        x_copy(1).start()

        def rest(cols, c):
            new = update(ur[:, cols], ADAPTER_SCALING * mm(lut[...], dpre[:, cols]), ur0[:, cols])
            ur[:, cols] = new
            urb[:, cols] = new.astype(BF16)
            new = update(dl[:, cols], mm(dld_t, act[:, cols]), dl0[:, cols])
            dl[:, cols] = new
            dlb[:, cols] = new.astype(BF16)
            return c
        tiles(rest, 0, UNROLL)

        def right(s):
            new = update(drp[s], ADAPTER_SCALING * mm(ldt[...], dout[s]), dr0p[s])
            drp[s] = new
            drb[s] = new.astype(BF16)
        each_slot(right)

    def end_left():
        x_copy(1).wait_recv()
        dlu_t = (xtx[1] + xrx[1]).astype(BF16)

        def left(s):
            new = update(ulp[s], mm(dlu_t, nx[s]), ul0p[s])
            ulp[s] = new
            ulb[s] = new.astype(BF16)
        each_slot(left)
        x_copy(0).wait_send()
        x_copy(1).wait_send()

        @pl.loop(0, R)
        def _(s):
            p_copy(s).wait_send()

    first_base()

    @pl.loop(1, R - 1)
    def _(s):
        advance(0, s, True)

        @pl.when(s == 1)
        def _():
            tiles(turned)

        @pl.when(s > 1)
        def _():
            add_base(s - 1)
    send_own(1)
    advance(0, R - 1, False)
    if R > 2:
        add_base(R - 2)
    add_base(R - 1)

    weight = count[0].astype(F32)
    cntb[me] = jnp.full(cntb.shape[1:], weight, F32)

    def cnt_copy(k):
        return copy(cntb.at[me], cntb.at[me], c_s.at[k], c_r.at[me], k, tp)

    @pl.loop(1, n)
    def _(i):
        cnt_copy((me + i) % n).start()
    advance(1, 1, R > 2)
    def pack(b, i0, per, change):
        owner, i = divmod(b, per)
        c, k = divmod(owner, R)
        sbuf[c, k, i0 + i] = (weight * change).astype(BF16)

    def wide_block(anchor, value, at):
        bits = []
        for lo in range(at, at + LANES, half):
            k, d = lo // rows, lo % rows // half
            where = (slot_of(k, d), slice(None), lanes_of(k, d))
            bits.append(anchor[where] - value[where])
        return jnp.concatenate(bits, axis=1)

    d = R * cr
    spans = (pl.ds(0, bpa), pl.ds(bpa, bpb))

    def pair(q):
        return copy(sbuf.at[1 - core, :, spans[q]], abuf.at[:, spans[q]], ab_s.at[q], ab_r.at[q], sib, tp)
    def chip_copy(q, k):
        return copy(bbuf.at[k, spans[q]], cbuf.at[chip, spans[q]], b_s.at[q, k], b_r.at[q, chip], k * 2 + core, tp)

    def chip_arrived(q, k):
        copy(bbuf.at[k, spans[q]], cbuf.at[k, spans[q]], b_s.at[q, k], b_r.at[q, k], k * 2 + core, tp).wait_recv()

    def back_copy(q, k):
        ref = rbuf.at[core, chip, spans[q]]
        return copy(ref, ref, g_s.at[q, k], g_r.at[q, chip], k * 2 + core, tp)

    def back_arrived(q, k):
        ref = rbuf.at[core, k, spans[q]]
        copy(ref, ref, g_s.at[q, k], g_r.at[q, k], k * 2 + core, tp).wait_recv()

    def pass_copy(q, c, k):
        ref = rbuf.at[c, k, spans[q]]
        return copy(ref, ref, f_s.at[q, k], f_r.at[q, k], sib, tp)

    def to_chips(q):
        pair(q).wait_recv()

        @pl.loop(0, R)
        def _(i):
            k = (chip + 1 + i) % R
            bbuf[k, spans[q]] = (sbuf[core, k, spans[q]].astype(F32) + abuf[k, spans[q]].astype(F32)).astype(BF16)

            @pl.when(i < R - 1)
            def _():
                chip_copy(q, k).start()
        cbuf[chip, spans[q]] = bbuf[chip, spans[q]]

    def last_sums():
        b = 0
        for value, anchor in ((ur, ur0), (dl, dl0)):
            for at in range(0, ffl, LANES):
                pack(b, 0, bpa, anchor[:, at:at + LANES] - value[:, at:at + LANES])
                b += 1

        for at in range(0, d, LANES):
            pack(b, 0, bpa, wide_block(dr0p, drp, at))
            b += 1
        for b in range(b, n * bpa):
            pack(b, 0, bpa, jnp.zeros(sbuf.shape[3:], F32))
        pair(0).start()

        to_chips(0)


    def gather_middle():
        sib_arrived(1, 0)
        forward_piece(0)
        p_copy(0).start()
        take_low()

        @pl.loop(2, R + 1)
        def _(s):
            @pl.when(s < R - 1)
            def _():
                advance(1, s, True)

            @pl.when(s == R - 1)
            def _():
                advance(1, s, False)
            sib_arrived(1, s - 1)
            forward_piece(s - 1)
            p_copy(s - 1).start()
            output_piece(s - 2)

            @pl.when(s == 2)
            def _():
                backward(0, 1, True)

            @pl.when(s > 2)
            def _():
                backward(s - 2, 1, False)
        output_piece(R - 1)

    def middle(t):
        held = t == 1

        @pl.loop(0, R)
        def _(s):
            forward_piece(s)

            @pl.when(jnp.logical_not(held & (core == 1)))
            def _():
                p_copy(s).start()

        @pl.when(held & (core == 1))
        def _():
            pl.semaphore_wait(turn, 1)

            @pl.loop(0, R)
            def _(s):
                p_copy(s).start()
        take_low()
        s0 = 0
        for g in groups:
            @pl.loop(s0, s0 + g)
            def _(s):
                output_piece(s)
            if s0 + g < R:
                backward(s0, g, s0 == 0)
            if s0 == groups[0]:
                @pl.when(held & (core == 0))
                def _():
                    pl.semaphore_signal(turn, inc=1, device_id={"client": sib, "tp": tp},
                                        device_id_type=pl.DeviceIdType.MESH)
            s0 += g

    def step(t):
        begin_step()
        pl.when(t == 0)(gather_middle)
        pl.when(t > 0)(functools.partial(middle, t))
        end_step(R - 1, 1)

    @pl.loop(0, STEPS)
    def _(t):
        step(t)
        pl.when(t == STEPS - 1)(last_sums)
        end_left()

    b = 0
    for at in range(0, d, LANES):
        pack(b, bpa, bpb, wide_block(ul0p, ulp, at))
        b += 1
    for b in range(b, n * bpb):
        pack(b, bpa, bpb, jnp.zeros(sbuf.shape[3:], F32))
    pair(1).start()

    @pl.loop(1, n)
    def _(i):
        k = (me + i) % n
        copy(cntb.at[k], cntb.at[k], c_s.at[k], c_r.at[k], k, tp).wait_recv()
    total = lax.fori_loop(0, n, lambda k, c: c + cntb[k], jnp.zeros(cntb.shape[1:], F32))
    factor = LEARN_RATE * total[0:1, 0:1]
    to_chips(1)
    for q in range(2):
        @pl.loop(1, R)
        def _(i):
            chip_arrived(q, (chip + i) % R)
        s = lax.fori_loop(0, R, lambda k, c: c + cbuf[k, spans[q]].astype(F32),
                          jnp.zeros((spans[q].size,) + cbuf.shape[2:], F32))
        rbuf[core, chip, spans[q]] = (s / factor).astype(BF16)

        @pl.loop(1, R)
        def _(i):
            back_copy(q, (chip + i) % R).start()
        pass_copy(q, core, chip).start()
    for q in range(2):
        @pl.loop(1, R)
        def _(i):
            k = (chip + i) % R
            back_arrived(q, k)
            pass_copy(q, core, k).start()
    for q in range(2):
        @pl.loop(0, R)
        def _(k):
            pass_copy(q, 1 - core, k).wait_recv()
    res[...] = rbuf[...]

    for q in range(2):
        pair(q).wait_send()

        @pl.loop(1, R)
        def _(i):
            k = (chip + i) % R
            chip_copy(q, k).wait_send()
            back_copy(q, k).wait_send()

        @pl.loop(0, R)
        def _(k):
            pass_copy(q, core, k).wait_send()

    @pl.loop(1, n)
    def _(i):
        cnt_copy((me + i) % n).wait_send()
    for m in range(2):
        for d, u in parts:
            @pl.loop(0, R)
            def _(s):
                sib_copy(m, d, s, u, core).wait_send()

            @pl.loop(0, R - 1)
            def _(s):
                ring_copy(m, d, s, u).wait_send()


def spread(n, bpa, bpb, res, oul, our, odl, odr):
    R = n // 2

    def take(b, i0, per, out, at):
        owner, i = divmod(b, per)
        c, k = divmod(owner, R)
        out[:, at:at + LANES] = res[c, k, i0 + i].astype(F32)
    b = 0
    for out in (our, odl, odr):
        for at in range(0, out.shape[1], LANES):
            take(b, 0, bpa, out, at)
            b += 1
    for b, at in enumerate(range(0, oul.shape[1], LANES)):
        take(b, bpa, bpb, oul, at)


def per_device(n, tokens, targets, norm_gain, up_frozen, down_frozen,
               up_left, up_right, down_left, down_right, counts):
    R = n // 2
    tok, d = tokens.shape
    rank = up_left.shape[0]
    rows, ffl = up_frozen.shape
    cr = 2 * rows
    subs = 2 if rows % 64 == 0 else 1
    tile = 512 if ffl % 512 == 0 else 128
    groups, left = [], R
    while left > 1:
        groups.append(min(4, left // 2))
        left -= groups[-1]
    groups.append(1)
    bpa = -(-(2 * ffl + d) // (LANES * n))
    bpb = -(-d // (LANES * n))
    bpd = bpa + bpb
    vm = pl.BlockSpec(memory_space=pltpu.VMEM)
    sm = pl.BlockSpec(memory_space=pltpu.SMEM)
    hbm = pl.BlockSpec(memory_space=pl.ANY)
    V = pltpu.VMEM
    dma = lambda *s: pltpu.SemaphoreType.DMA(s)
    packed = pl.pallas_call(
        functools.partial(kernel, n, subs, bpa, bpb, tile, tuple(groups)),
        out_shape=jax.ShapeDtypeStruct((2, R, bpd, rank, LANES), BF16),
        in_specs=[hbm] * 9 + [sm],
        out_specs=vm,
        scratch_shapes=[
            V((R, cr, ffl), BF16), V((R, cr, ffl), BF16),
            V((tok, ffl), F32), V((tok, ffl), F32), V((tok, ffl), F32),
            V((tok, ffl), BF16), V((tok, ffl), BF16),
            V((R, tok, cr), BF16), V((R, tok, cr), BF16), V((R, tok, cr), BF16),
            V((R, tok, cr), BF16), V((R, tok, cr), F32),
            V((ffl, rows), BF16), V((1, d), F32),
            V((rank, d), F32), V((rank, ffl), F32), V((rank, ffl), F32), V((rank, d), F32),
            V((R, rank, cr), F32), V((R, rank, cr), F32), V((R, rank, cr), F32), V((R, rank, cr), F32),
            V((rank, ffl), F32), V((rank, ffl), F32),
            V((R, rank, cr), BF16), V((R, rank, cr), BF16), V((rank, ffl), BF16), V((rank, ffl), BF16),
            V((rank, tok), BF16), V((rank, tok), BF16), V((rank, tok), F32), V((tok, rank), BF16),
            V((2, rank, tok), F32), V((2, rank, tok), F32), V((n, 8, LANES), F32),
            V((2, R, bpd, rank, LANES), BF16), V((R, bpd, rank, LANES), BF16),
            V((R, bpd, rank, LANES), BF16), V((R, bpd, rank, LANES), BF16),
            V((2, R, bpd, rank, LANES), BF16),
            dma(2, subs), dma(8), dma(2, 2, R, subs), dma(2, 2, R, subs), dma(2, 2, R, subs), dma(2, 2, R, subs),
            dma(R), dma(R), dma(2), dma(2), dma(n), dma(n),
            dma(2), dma(2), dma(2, R), dma(2, R), dma(2, R), dma(2, R), dma(2, R), dma(2, R),
            pltpu.SemaphoreType.REGULAR,
        ],
        compiler_params=pltpu.CompilerParams(
            vmem_limit_bytes=65400 * 1024, has_side_effects=True, collective_id=0),
    )(up_frozen, down_frozen, tokens, targets, norm_gain.reshape(1, d),
      up_left, up_right, down_left, down_right, counts)
    return pl.pallas_call(
        functools.partial(spread, n, bpa, bpb),
        out_shape=[jax.ShapeDtypeStruct(a.shape, F32)
                   for a in (up_left, up_right, down_left, down_right)],
        in_specs=[vm],
        out_specs=[vm] * 4,
    )(packed)


def solution(mesh):
    placed = (
        P("client", None),
        P("client", None),
        P(),
        P("client", "tp"),
        P("tp", "client"),
        P(),
        P(None, "tp"),
        P(None, "tp"),
        P(),
        P("client"),
    )
    return jax.shard_map(
        functools.partial(per_device, mesh.shape["client"]),
        mesh=mesh,
        in_specs=placed,
        out_specs=(P(), P(None, "tp"), P(None, "tp"), P()),
        check_vma=False,
    )
```
